128 devices in a mesh: rep: 1, dp: 128 (over x, y, z, core).
Axes of the slice: x: 4, y: 4, z: 4, core: 2. Of those that a mesh axis runs over, the one named last changes fastest.
Arguments:
- a: bfloat16 [128, 2, 4096, 1280], P(('rep', 'dp'))
- g: bfloat16 [128, 2, 4096, 3584], P(('rep', 'dp'))
Outputs:
- output: bfloat16 [2, 1280, 3584], P('rep')
All inputs are finite; a program needn't handle non-finite values.
Results may differ from the reference program's by a relative error of at most 0.012.
Values are sent between devices in bfloat16 or wider.
A program may use at most 1.5 GiB of HBM per device.

```python
import jax
import jax.numpy as jnp
from jax import lax

DEVICES = 128
MATRICES = 2
TOKENS = 4096
D = 1280
FF = 3584


def setup_inputs(seed: int = 0, part: int = 0) -> dict:
    ka, kg, ks = (jax.random.fold_in(k, part) for k in jax.random.split(jax.random.key(seed), 3))
    size = 2.0 ** jax.random.uniform(ks, (DEVICES, MATRICES, 1, 1), jnp.float32, -1.0, 1.0)
    a = jax.random.normal(ka, (DEVICES, MATRICES, TOKENS, D), jnp.float32)
    g = size * jax.random.normal(kg, (DEVICES, MATRICES, TOKENS, FF), jnp.float32) * (DEVICES * TOKENS) ** -0.5
    return {"a": a.astype(jnp.bfloat16), "g": g.astype(jnp.bfloat16)}


def reference(a, g):
    def take(so_far, one):
        term = jnp.einsum("ntd,ntf->ndf", *one, preferred_element_type=jnp.float32).astype(jnp.bfloat16)
        return so_far + term.astype(jnp.float32), None

    return lax.scan(take, jnp.zeros((MATRICES, D, FF), jnp.float32), (a, g))[0].astype(jnp.bfloat16)
```

```python
import jax
import jax.numpy as jnp
from jax import lax
from jax.experimental import pallas as pl
from jax.experimental.pallas import tpu as pltpu
from jax.sharding import PartitionSpec as P

N, D, F, K = 2, 1280, 3584, 4096
NB = 512
NC = F // NB
CH = N * NC
H = D // 2
RB = H // 4
CB = NB // 4
HB = RB // 2
HC = NB // 2

F32, BF16 = jnp.float32, jnp.bfloat16

OFF = {2: 2, 3: 5, 4: 7, 5: 9, 6: 11, 7: 13, 8: 15, 9: 17, 10: 20, 11: 22}
LAST = CH + (OFF[11] + 1) // 2 + 1


def kernel(a_ref, g_ref, out, av, gv, fs, fb, d2d, ra1, ra2, rb1, rb2, rc,
           sem_a, sem_g, s_d, r_d, s_x, r_d2, ss, rs, free):
    me = lax.axis_index("dp")
    core = me % 2
    partner = me + 1 - 2 * core
    mine = pl.multiple_of(core * H, H)
    theirs = pl.multiple_of((1 - core) * H, H)

    def axis(k):
        stride = 32 - 33 * k + 9 * k * k
        return (me // stride) % 4, stride

    def dev(k, d):
        c, stride = axis(k)
        return me + ((c + d + 4) % 4 - c) * stride

    def rdma(src, dst, s, r, to):
        return pltpu.make_async_remote_copy(
            src_ref=src, dst_ref=dst, send_sem=s, recv_sem=r,
            device_id={"dp": to}, device_id_type=pl.DeviceIdType.MESH)

    def acopy(n):
        return pltpu.make_async_copy(a_ref.at[0, n], av.at[n], sem_a.at[n])

    def gcopy(t):
        n, c = t // NC, t % NC
        cols = pl.ds(pl.multiple_of(c * NB, NB), NB)
        return pltpu.make_async_copy(g_ref.at[0, n, :, cols], gv.at[t % 2], sem_g.at[t % 2])

    acopy(0).start()
    gcopy(0).start()
    acopy(1).start()

    barrier = pltpu.get_barrier_semaphore()
    pl.semaphore_signal(barrier, inc=1, device_id={"dp": partner}, device_id_type=pl.DeviceIdType.MESH)
    for k in range(3):
        for d in (1, -1):
            pl.semaphore_signal(barrier, inc=1, device_id={"dp": dev(k, d)},
                                device_id_type=pl.DeviceIdType.MESH)
    pl.semaphore_wait(barrier, 7)

    acopy(0).wait()

    def dot(n, t, rows):
        return lax.dot_general(av[n, :, pl.ds(rows, H)], gv[t % 2], (((0,), (0,)), ((), ())),
                               preferred_element_type=F32)

    class Chunk:
        def __init__(self, t):
            self.t = t
            self.n, c = t // NC, t % NC
            self.col = pl.multiple_of(c * NB, NB)
            self.r = t % 3
            self.s3, self.s6 = t % 3, t % 6

        def ax(self, i):
            return (self.r + i) % 3

        def pos(self, i, d):
            return (axis(self.ax(i))[0] + d + 4) % 4

        def dev(self, i, d):
            return dev(self.ax(i), d)

        def block(self, d, half=None):
            rows = pl.ds(pl.multiple_of(mine + self.pos(0, d) * RB, RB), RB)
            if half is None:
                return out.at[self.n, rows, pl.ds(self.col, NB)]
            return out.at[self.n, rows, pl.ds(pl.multiple_of(self.col + half * HC, HC), HC)]

        def rel(self, d):
            return pl.ds(pl.multiple_of(self.pos(0, d) * RB, RB), RB)

        def sub(self, d, half=None):
            r0 = mine + self.pos(0, 0) * RB
            cols = pl.ds(pl.multiple_of(self.col + self.pos(1, d) * CB, CB), CB)
            if half is None:
                return out.at[self.n, pl.ds(pl.multiple_of(r0, RB), RB), cols]
            return out.at[self.n, pl.ds(pl.multiple_of(r0 + half * HB, HB), HB), cols]

        def relc(self, d):
            return pl.ds(pl.multiple_of(self.pos(1, d) * CB, CB), CB)

        def copies(self, st):
            s3, s6 = self.s3, self.s6
            if st == 1:
                i, p = 0, ((self.block(2, 0), ra1.at[s3, 0]), (self.block(2, 1), ra1.at[s3, 1]))
            elif st == 2:
                i, p = 0, ((self.block(1), ra2.at[s3, 0]), (self.block(-1), ra2.at[s3, 1]))
            elif st == 3:
                i, p = 1, ((self.sub(2, 0), rb1.at[s3, 0]), (self.sub(2, 1), rb1.at[s3, 1]))
            elif st == 4:
                i, p = 1, ((self.sub(1), rb2.at[s3, 0]), (self.sub(-1), rb2.at[s3, 1]))
            elif st == 5:
                i, p = 2, ((self.sub(0), rc.at[s6, 0]), (self.sub(0), rc.at[s6, 1]))
            elif st == 6:
                up, lo = pl.ds(0, HB), pl.ds(HB, HB)
                i, p = 2, ((rc.at[s6, 0, up], rc.at[s6, 2, up]), (rc.at[s6, 1, lo], rc.at[s6, 2, lo]))
            elif st == 7:
                i, p = 1, ((self.sub(0), self.sub(0)), (self.sub(0), self.sub(0)))
            elif st == 8:
                i, p = 1, ((self.sub(-1, 0), self.sub(-1, 0)), (self.sub(1, 1), self.sub(1, 1)))
            elif st == 9:
                i, p = 0, ((self.block(0), self.block(0)), (self.block(0), self.block(0)))
            elif st == 10:
                i, p = 0, ((self.block(-1, 0), self.block(-1, 0)), (self.block(1, 1), self.block(1, 1)))
            return [rdma(src, dst, ss.at[st - 1, j, s6], rs.at[st - 1, j, s6], self.dev(i, d))
                    for j, (d, (src, dst)) in enumerate(zip((1, -1), p))]

        def send(self, st):
            for c in self.copies(st):
                c.start()

        def wait(self, st):
            for c in self.copies(st):
                c.wait_send()
            for c in self.copies(st):
                c.wait_recv()

        def send_theirs(self):
            src = out.at[self.n, pl.ds(theirs, H), pl.ds(self.col, NB)]
            return rdma(src, d2d.at[self.t % 5], s_d.at[self.t % 5], r_d.at[self.t % 5], partner)

        def send_mine(self):
            src = out.at[self.n, pl.ds(mine, H), pl.ds(self.col, NB)]
            return rdma(src, src, s_x.at[self.t], r_d2.at[self.t], partner)

        def give(self, i):
            for j, d in enumerate((1, -1)):
                pl.semaphore_signal(free.at[i, j, self.s6], inc=1, device_id={"dp": self.dev(i, d)},
                                    device_id_type=pl.DeviceIdType.MESH)

        def take(self, i):
            for j in range(2):
                pl.semaphore_wait(free.at[i, j, self.s6], 1)

        def chip(self, d):
            rows = self.rel(d)
            return fs[self.s3, rows, :] + d2d[self.t % 5, rows, :].astype(F32)

        def stage(self, st):
            self.wait(st - 1)
            s3, s6 = self.s3, self.s6
            if st == 2:
                v = self.chip(1)
                self.block(1, 0)[...] = (v[:, :HC] + ra1[s3, 0].astype(F32)).astype(BF16)
                self.block(1, 1)[...] = v[:, HC:].astype(BF16)
                v = self.chip(-1)
                self.block(-1, 0)[...] = v[:, :HC].astype(BF16)
                self.block(-1, 1)[...] = (v[:, HC:] + ra1[s3, 1].astype(F32)).astype(BF16)
            elif st == 3:
                fb[s3] = self.chip(0) + ra2[s3, 0].astype(F32) + ra2[s3, 1].astype(F32)
                self.sub(2)[...] = fb[s3, :, self.relc(2)].astype(BF16)
            elif st == 4:
                v = fb[s3, :, self.relc(1)]
                self.sub(1, 0)[...] = (v[:HB] + rb1[s3, 0].astype(F32)).astype(BF16)
                self.sub(1, 1)[...] = v[HB:].astype(BF16)
                v = fb[s3, :, self.relc(-1)]
                self.sub(-1, 0)[...] = v[:HB].astype(BF16)
                self.sub(-1, 1)[...] = (v[HB:] + rb1[s3, 1].astype(F32)).astype(BF16)
            elif st == 5:
                v = fb[s3, :, self.relc(0)]
                self.sub(0)[...] = (v + rb2[s3, 0].astype(F32) + rb2[s3, 1].astype(F32)).astype(BF16)
            elif st == 7:
                even = self.sub(0)[...].astype(F32) + rc[s6, 2].astype(F32)
                odd = rc[s6, 0].astype(F32) + rc[s6, 1].astype(F32)
                self.sub(0)[...] = (even + odd).astype(BF16)
            if st == 3:
                self.give(0)
            elif st == 5:
                self.give(1)
            elif st == 7:
                self.take(1)
            elif st == 9:
                self.take(0)
            if st <= 10:
                self.send(st)
            else:
                pl.semaphore_wait(free.at[2, 0, s6], 1)
                self.send_mine().start()

    def slot(t, half):
        for st in range(11, 1, -1):
            off = OFF[st]
            if half == 1 and off % 2 == 0:
                u = t - off // 2
            elif half == 0 and off % 2 == 1:
                u = t - (1 + off) // 2
            else:
                continue

            @pl.when(jnp.logical_and(u >= 0, u < CH))
            def _():
                Chunk(u).stage(st)

    def body(t, _):
        c = Chunk(t)

        @pl.when(t < CH)
        def _():
            @pl.when(t + 1 < CH)
            def _():
                gcopy(t + 1).start()
            gcopy(t).wait()

            @pl.when(t == NC)
            def _():
                acopy(1).wait()

            out[c.n, pl.ds(theirs, H), pl.ds(c.col, NB)] = dot(c.n, t, theirs).astype(BF16)
            c.send_theirs().start()

        slot(t, 0)

        @pl.when(t < CH)
        def _():
            fs[c.s3] = dot(c.n, t, mine)
            w = c.send_theirs()
            w.wait_send()
            pl.semaphore_signal(free.at[2, 0, c.s6], inc=1, device_id={"dp": partner},
                                device_id_type=pl.DeviceIdType.MESH)
            w.wait_recv()
            c.block(2)[...] = c.chip(2).astype(BF16)
            c.send(1)

        slot(t, 1)
        return 0

    lax.fori_loop(0, LAST, body, 0)

    def drain(t, _):
        c = Chunk(t).send_mine()
        c.wait_send()
        c.wait_recv()
        return 0

    lax.fori_loop(0, CH, drain, 0)


def local(a, g):
    dma = pltpu.SemaphoreType.DMA
    return pl.pallas_call(
        kernel,
        out_shape=pltpu.VMEM((N, D, F), BF16),
        in_specs=[pl.BlockSpec(memory_space=pl.ANY)] * 2,
        out_specs=pl.BlockSpec(memory_space=pltpu.VMEM),
        scratch_shapes=[
            pltpu.VMEM((N, K, D), BF16),
            pltpu.VMEM((2, K, NB), BF16),
            pltpu.VMEM((3, H, NB), F32),
            pltpu.VMEM((3, RB, NB), F32),
            pltpu.VMEM((5, H, NB), BF16),
            pltpu.VMEM((3, 2, RB, HC), BF16),
            pltpu.VMEM((3, 2, RB, NB), BF16),
            pltpu.VMEM((3, 2, HB, CB), BF16),
            pltpu.VMEM((3, 2, RB, CB), BF16),
            pltpu.VMEM((6, 3, RB, CB), BF16),
            dma((2,)), dma((2,)), dma((5,)), dma((5,)), dma((CH,)), dma((CH,)),
            dma((10, 2, 6)), dma((10, 2, 6)), pltpu.SemaphoreType.REGULAR((3, 2, 6)),
        ],
        compiler_params=pltpu.CompilerParams(
            collective_id=0, has_side_effects=True, vmem_limit_bytes=46 * 2**20),
        name="wgrad_sum",
    )(a, g)


def solution(mesh):
    spec = P(("rep", "dp"))
    return jax.shard_map(local, mesh=mesh, in_specs=(spec, spec), out_specs=P("rep"), check_vma=False)
```

```python
import jax
import jax.numpy as jnp
from jax import lax
from jax.experimental import pallas as pl
from jax.experimental.pallas import tpu as pltpu
from jax.sharding import PartitionSpec as P

N, D, F, K = 2, 1280, 3584, 4096
NB = 512
NC = F // NB
CH = N * NC
H = D // 2
RB = H // 4
CB = NB // 4
FC = NB // 4
PEERS = (1, 2, -1)

F32, BF16 = jnp.float32, jnp.bfloat16

OFF = {2: 2, 3: 5, 4: 7, 5: 9, 6: 11, 7: 14, 8: 16}
LAST = CH + (OFF[8] + 1) // 2 + 1


def kernel(a_ref, g_ref, out, av, gv, fs, fb, d2d, ra1, ra2, rb, rc,
           sem_a, sem_g, s_d, r_d, s_x, r_d2, ss, rs, free):
    me = lax.axis_index("dp")
    core = me % 2
    partner = me + 1 - 2 * core
    mine = pl.multiple_of(core * H, H)
    theirs = pl.multiple_of((1 - core) * H, H)

    place, device = [], []
    for stride in (32, 8, 2):
        c = (me // stride) % 4
        place.append({d: (c + d + 4) % 4 for d in (-1, 0, 1, 2)})
        device.append({d: me + (place[-1][d] - c) * stride for d in PEERS})

    def pick(k, of, d):
        return jnp.where(k == 0, of[0][d], jnp.where(k == 1, of[1][d], of[2][d]))

    def rdma(src, dst, s, r, to):
        return pltpu.make_async_remote_copy(
            src_ref=src, dst_ref=dst, send_sem=s, recv_sem=r,
            device_id={"dp": to}, device_id_type=pl.DeviceIdType.MESH)

    def acopy(n, rows):
        cols = pl.ds(rows, H)
        return pltpu.make_async_copy(a_ref.at[0, n, :, cols], av.at[n, :, cols], sem_a.at[n, (0 if rows is theirs else 1)])

    def split(t):
        n = jnp.where(t >= NC, 1, 0)
        return n, t - n * NC

    def gcopy(t):
        n, c = split(t)
        cols = pl.ds(pl.multiple_of(c * NB, NB), NB)
        b = lax.rem(t, 2)
        return pltpu.make_async_copy(g_ref.at[0, n, :, cols], gv.at[b], sem_g.at[b])

    gcopy(0).start()
    acopy(0, theirs).start()
    acopy(0, mine).start()

    barrier = pltpu.get_barrier_semaphore()
    pl.semaphore_signal(barrier, inc=1, device_id={"dp": partner}, device_id_type=pl.DeviceIdType.MESH)
    for k in range(3):
        for d in PEERS:
            pl.semaphore_signal(barrier, inc=1, device_id={"dp": device[k][d]},
                                device_id_type=pl.DeviceIdType.MESH)
    pl.semaphore_wait(barrier, 10)

    def dot(n, t, rows):
        return lax.dot_general(av[n, :, pl.ds(rows, H)], gv[lax.rem(t, 2)], (((0,), (0,)), ((), ())),
                               preferred_element_type=F32)

    class Chunk:
        def __init__(self, t, s6):
            self.t = t
            self.n, c = split(t)
            self.col = pl.multiple_of(c * NB, NB)
            self.s6 = s6
            self.s3 = jnp.where(s6 >= 3, s6 - 3, s6)

        def ax(self, i):
            k = self.s3 + core + i
            return jnp.where(k >= 3, k - 3, k)

        def pos(self, i, d):
            return pick(self.ax(i), place, d)

        def dev(self, i, d):
            return pick(self.ax(i), device, d)

        def block(self, d, lo=0, n=NB):
            rows = pl.ds(pl.multiple_of(mine + self.pos(0, d) * RB, RB), RB)
            return out.at[self.n, rows, pl.ds(pl.multiple_of(self.col + lo, CB), n)]

        def rel(self, d):
            return pl.ds(pl.multiple_of(self.pos(0, d) * RB, RB), RB)

        def sub(self, d):
            rows = pl.ds(pl.multiple_of(mine + self.pos(0, 0) * RB, RB), RB)
            return out.at[self.n, rows, pl.ds(pl.multiple_of(self.col + self.pos(1, d) * CB, CB), CB)]

        def relc(self, d):
            return pl.ds(pl.multiple_of(self.pos(1, d) * CB, CB), CB)

        def copies(self, st):
            s3, s6 = self.s3, self.s6
            lo, hi = pl.ds(0, FC), pl.ds(FC, NB - FC)
            if st == 1:
                i, p = 0, ((1, self.block(2, 0, FC), ra1.at[s3, :, lo]),
                           (-1, self.block(2, FC, NB - FC), ra1.at[s3, :, hi]))
            elif st == 2:
                i, p = 0, ((1, self.block(1), ra2.at[s3, 0]), (-1, self.block(-1), ra2.at[s3, 1]))
            elif st == 3:
                i, p = 1, [(d, self.sub(d), rb.at[s3, j]) for j, d in enumerate(PEERS)]
            elif st == 4:
                i, p = 2, [(d, self.sub(0), rc.at[s6, j]) for j, d in enumerate(PEERS)]
            elif st == 5:
                i, p = 1, [(d, self.sub(0), self.sub(0)) for d in PEERS]
            elif st == 6:
                i, p = 0, [(d, self.block(0), self.block(0)) for d in (1, -1)]
            elif st == 7:
                fwd, bwd = self.block(-1, 0, FC), self.block(1, FC, NB - FC)
                i, p = 0, ((1, fwd, fwd), (-1, bwd, bwd))
            return [rdma(src, dst, ss.at[st - 1, j, s6], rs.at[st - 1, j, s6], self.dev(i, d))
                    for j, (d, src, dst) in enumerate(p)]

        def send(self, st):
            for c in self.copies(st):
                c.start()

        def wait(self, st):
            copies = self.copies(st)
            for c in copies:
                c.wait_send()
            for c in copies:
                c.wait_recv()

        def send_theirs(self):
            src = out.at[self.n, pl.ds(theirs, H), pl.ds(self.col, NB)]
            return rdma(src, d2d.at[self.s6], s_d.at[self.s6], r_d.at[self.s6], partner)

        def send_mine(self):
            src = out.at[self.n, pl.ds(mine, H), pl.ds(self.col, NB)]
            return rdma(src, src, s_x.at[self.t], r_d2.at[self.t], partner)

        def give(self, i, peers):
            for j, d in enumerate(peers):
                pl.semaphore_signal(free.at[i, j, self.s6], inc=1, device_id={"dp": self.dev(i, d)},
                                    device_id_type=pl.DeviceIdType.MESH)

        def take(self, i, n):
            for j in range(n):
                pl.semaphore_wait(free.at[i, j, self.s6], 1)

        def chip(self, d):
            rows = self.rel(d)
            return fs[self.s3, rows, :] + d2d[self.s6, rows, :].astype(F32)

        def stage(self, st):
            self.wait(st - 1)
            s3, s6 = self.s3, self.s6
            if st == 2:
                v = self.chip(1)
                self.block(1, 0, FC)[...] = (v[:, :FC] + ra1[s3, :, :FC].astype(F32)).astype(BF16)
                self.block(1, FC, NB - FC)[...] = v[:, FC:].astype(BF16)
                v = self.chip(-1)
                self.block(-1, 0, FC)[...] = v[:, :FC].astype(BF16)
                self.block(-1, FC, NB - FC)[...] = (v[:, FC:] + ra1[s3, :, FC:].astype(F32)).astype(BF16)
            elif st == 3:
                fb[s3] = self.chip(0) + ra2[s3, 0].astype(F32) + ra2[s3, 1].astype(F32)
                for d in PEERS:
                    self.sub(d)[...] = fb[s3, :, self.relc(d)].astype(BF16)
                self.give(0, (1, -1))
            elif st == 4:
                v = fb[s3, :, self.relc(0)]
                for j in range(3):
                    v = v + rb[s3, j].astype(F32)
                self.sub(0)[...] = v.astype(BF16)
                self.give(1, PEERS)
            elif st == 5:
                even = self.sub(0)[...].astype(F32) + rc[s6, 1].astype(F32)
                odd = rc[s6, 0].astype(F32) + rc[s6, 2].astype(F32)
                self.sub(0)[...] = (even + odd).astype(BF16)
                self.take(1, 3)
            elif st == 6:
                self.take(0, 2)
            if st <= 7:
                self.send(st)
            else:
                pl.semaphore_wait(free.at[2, 0, s6], 1)
                self.send_mine().start()

    def slot(t, t6, half):
        for st in range(8, 1, -1):
            off = OFF[st]
            if half == 1 and off % 2 == 0:
                back = off // 2
            elif half == 0 and off % 2 == 1:
                back = (1 + off) // 2
            else:
                continue
            u, u6 = t - back, t6 - back % 6

            @pl.when(jnp.logical_and(u >= 0, u < CH))
            def _():
                Chunk(u, jnp.where(u6 < 0, u6 + 6, u6)).stage(st)

    def body(t, t6):
        c = Chunk(t, t6)

        @pl.when(t < CH)
        def _():
            @pl.when(t + 1 < CH)
            def _():
                gcopy(t + 1).start()
            gcopy(t).wait()

            @pl.when(c.col == 0)
            def _():
                acopy(c.n, theirs).wait()

            out[c.n, pl.ds(theirs, H), pl.ds(c.col, NB)] = dot(c.n, t, theirs).astype(BF16)
            c.send_theirs().start()

        slot(t, t6, 0)

        @pl.when(t < CH)
        def _():
            @pl.when(c.col == 0)
            def _():
                acopy(c.n, mine).wait()

            @pl.when(t == 1)
            def _():
                acopy(1, theirs).start()
                acopy(1, mine).start()

            fs[c.s3] = dot(c.n, t, mine)
            w = c.send_theirs()
            w.wait_send()
            pl.semaphore_signal(free.at[2, 0, c.s6], inc=1, device_id={"dp": partner},
                                device_id_type=pl.DeviceIdType.MESH)
            w.wait_recv()
            c.block(2)[...] = c.chip(2).astype(BF16)
            c.send(1)

        slot(t, t6, 1)
        return jnp.where(t6 == 5, 0, t6 + 1)

    lax.fori_loop(0, LAST, body, 0)

    def drain(t, _):
        c = Chunk(t, 0).send_mine()
        c.wait_send()
        c.wait_recv()
        return 0

    lax.fori_loop(0, CH, drain, 0)


def local(a, g):
    dma = pltpu.SemaphoreType.DMA
    return pl.pallas_call(
        kernel,
        out_shape=pltpu.VMEM((N, D, F), BF16),
        in_specs=[pl.BlockSpec(memory_space=pl.ANY)] * 2,
        out_specs=pl.BlockSpec(memory_space=pltpu.VMEM),
        scratch_shapes=[
            pltpu.VMEM((N, K, D), BF16),
            pltpu.VMEM((2, K, NB), BF16),
            pltpu.VMEM((3, H, NB), F32),
            pltpu.VMEM((3, RB, NB), F32),
            pltpu.VMEM((6, H, NB), BF16),
            pltpu.VMEM((3, RB, NB), BF16),
            pltpu.VMEM((3, 2, RB, NB), BF16),
            pltpu.VMEM((3, 3, RB, CB), BF16),
            pltpu.VMEM((6, 3, RB, CB), BF16),
            dma((2, 2)), dma((2,)), dma((6,)), dma((6,)), dma((CH,)), dma((CH,)),
            dma((7, 3, 6)), dma((7, 3, 6)), pltpu.SemaphoreType.REGULAR((3, 3, 6)),
        ],
        compiler_params=pltpu.CompilerParams(
            collective_id=0, has_side_effects=True, vmem_limit_bytes=46 * 2**20),
        name="wgrad_sum",
    )(a, g)


def solution(mesh):
    spec = P(("rep", "dp"))
    return jax.shard_map(local, mesh=mesh, in_specs=(spec, spec), out_specs=P("rep"), check_vma=False)
```

```python
import jax
import jax.numpy as jnp
from jax import lax
from jax.experimental import pallas as pl
from jax.experimental.pallas import tpu as pltpu
from jax.sharding import PartitionSpec as P

N, D, F, K = 2, 1280, 3584, 4096
NB = 512
NC = F // NB
CH = N * NC
H = D // 2
RB = H // 4
CB = NB // 4
FC = NB // 4
PEERS = (1, 2, -1)
STRIP = 32

F32, BF16 = jnp.float32, jnp.bfloat16

OFF = {2: 2, 3: 5, 4: 7, 5: 9, 6: 11, 7: 13, 8: 15}
LAST = CH + (OFF[8] + 1) // 2 + 1


def kernel(a_ref, g_ref, out, av, gv, fs, fb, d2d, ra1, ra2, rb, rc,
           sem_a, sem_g, s_d, r_d, s_x, r_d2, ss, rs, free):
    me = lax.axis_index("dp")
    core = me % 2
    partner = me + 1 - 2 * core
    mine = pl.multiple_of(core * H, H)
    theirs = pl.multiple_of((1 - core) * H, H)

    place, device = [], []
    for stride in (32, 8, 2):
        c = (me // stride) % 4
        place.append({d: (c + d + 4) % 4 for d in (-1, 0, 1, 2)})
        device.append({d: me + (place[-1][d] - c) * stride for d in PEERS})

    def pick(k, of, d):
        return jnp.where(k == 0, of[0][d], jnp.where(k == 1, of[1][d], of[2][d]))

    def rdma(src, dst, s, r, to):
        return pltpu.make_async_remote_copy(
            src_ref=src, dst_ref=dst, send_sem=s, recv_sem=r,
            device_id={"dp": to}, device_id_type=pl.DeviceIdType.MESH)

    def acopy(n, rows):
        cols = pl.ds(rows, H)
        return pltpu.make_async_copy(a_ref.at[0, n, :, cols], av.at[n, :, cols], sem_a.at[n, (0 if rows is theirs else 1)])

    def split(t):
        n = jnp.where(t >= NC, 1, 0)
        return n, t - n * NC

    def gcopy(t):
        n, c = split(t)
        cols = pl.ds(pl.multiple_of(c * NB, NB), NB)
        b = lax.rem(t, 2)
        return pltpu.make_async_copy(g_ref.at[0, n, :, cols], gv.at[b], sem_g.at[b])

    gcopy(0).start()
    acopy(0, theirs).start()
    acopy(0, mine).start()

    barrier = pltpu.get_barrier_semaphore()
    pl.semaphore_signal(barrier, inc=1, device_id={"dp": partner}, device_id_type=pl.DeviceIdType.MESH)
    for k in range(3):
        for d in PEERS:
            pl.semaphore_signal(barrier, inc=1, device_id={"dp": device[k][d]},
                                device_id_type=pl.DeviceIdType.MESH)
    pl.semaphore_wait(barrier, 10)

    def dot(n, t, rows):
        return lax.dot_general(av[n, :, pl.ds(rows, H)], gv[lax.rem(t, 2)], (((0,), (0,)), ((), ())),
                               preferred_element_type=F32)

    def total(dst, *terms):
        for r in range(0, dst.shape[0], STRIP):
            rows = pl.ds(r, STRIP)
            v = terms[0][rows, :].astype(F32)
            for term in terms[1:]:
                v = v + term[rows, :].astype(F32)
            dst[rows, :] = v.astype(dst.dtype)

    class Chunk:
        def __init__(self, t, s6):
            self.t = t
            self.n, c = split(t)
            self.col = pl.multiple_of(c * NB, NB)
            self.s6 = s6
            self.s3 = jnp.where(s6 >= 3, s6 - 3, s6)

        def ax(self, i):
            k = self.s3 + core + i
            return jnp.where(k >= 3, k - 3, k)

        def pos(self, i, d):
            return pick(self.ax(i), place, d)

        def dev(self, i, d):
            return pick(self.ax(i), device, d)

        def block(self, d, lo=0, n=NB):
            rows = pl.ds(pl.multiple_of(mine + self.pos(0, d) * RB, RB), RB)
            return out.at[self.n, rows, pl.ds(pl.multiple_of(self.col + lo, CB), n)]

        def rel(self, d):
            return pl.ds(pl.multiple_of(self.pos(0, d) * RB, RB), RB)

        def sub(self, d):
            rows = pl.ds(pl.multiple_of(mine + self.pos(0, 0) * RB, RB), RB)
            return out.at[self.n, rows, pl.ds(pl.multiple_of(self.col + self.pos(1, d) * CB, CB), CB)]

        def relc(self, d):
            return pl.ds(pl.multiple_of(self.pos(1, d) * CB, CB), CB)

        def copies(self, st):
            s3, s6 = self.s3, self.s6
            lo, hi = pl.ds(0, FC), pl.ds(FC, NB - FC)
            if st == 1:
                i, p = 0, ((1, self.block(2, 0, FC), ra1.at[s3, :, lo]),
                           (-1, self.block(2, FC, NB - FC), ra1.at[s3, :, hi]))
            elif st == 2:
                i, p = 0, ((1, self.block(1), ra2.at[s3, 0]), (-1, self.block(-1), ra2.at[s3, 1]))
            elif st == 3:
                i, p = 1, [(d, self.sub(d), rb.at[s3, j]) for j, d in enumerate(PEERS)]
            elif st == 4:
                i, p = 2, [(d, self.sub(0), rc.at[s6, j]) for j, d in enumerate(PEERS)]
            elif st == 5:
                i, p = 1, [(d, self.sub(0), self.sub(0)) for d in PEERS]
            elif st == 6:
                i, p = 0, [(d, self.block(0), self.block(0)) for d in (1, -1)]
            elif st == 7:
                fwd, bwd = self.block(-1, 0, FC), self.block(1, FC, NB - FC)
                i, p = 0, ((1, fwd, fwd), (-1, bwd, bwd))
            return [rdma(src, dst, ss.at[st - 1, j, s6], rs.at[st - 1, j, s6], self.dev(i, d))
                    for j, (d, src, dst) in enumerate(p)]

        def send(self, st):
            for c in self.copies(st):
                c.start()

        def wait(self, st):
            copies = self.copies(st)
            for c in copies:
                c.wait_send()
            for c in copies:
                c.wait_recv()

        def send_theirs(self):
            src = out.at[self.n, pl.ds(theirs, H), pl.ds(self.col, NB)]
            return rdma(src, d2d.at[self.s6], s_d.at[self.s6], r_d.at[self.s6], partner)

        def send_mine(self):
            src = out.at[self.n, pl.ds(mine, H), pl.ds(self.col, NB)]
            return rdma(src, src, s_x.at[self.t], r_d2.at[self.t], partner)

        def give(self, i, peers):
            for j, d in enumerate(peers):
                pl.semaphore_signal(free.at[i, j, self.s6], inc=1, device_id={"dp": self.dev(i, d)},
                                    device_id_type=pl.DeviceIdType.MESH)

        def take(self, i, n):
            for j in range(n):
                pl.semaphore_wait(free.at[i, j, self.s6], 1)

        def chip(self, d, lo=0, n=NB):
            rows, cols = self.rel(d), pl.ds(lo, n)
            return fs.at[self.s3, rows, cols], d2d.at[self.s6, rows, cols]

        def stage(self, st):
            self.wait(st - 1)
            s3, s6 = self.s3, self.s6
            rest = NB - FC
            if st == 2:
                total(self.block(1, 0, FC), *self.chip(1, 0, FC), ra1.at[s3, :, pl.ds(0, FC)])
                total(self.block(1, FC, rest), *self.chip(1, FC, rest))
                total(self.block(-1, 0, FC), *self.chip(-1, 0, FC))
                total(self.block(-1, FC, rest), *self.chip(-1, FC, rest), ra1.at[s3, :, pl.ds(FC, rest)])
            elif st == 3:
                total(fb.at[s3], *self.chip(0), ra2.at[s3, 0], ra2.at[s3, 1])
                for d in PEERS:
                    total(self.sub(d), fb.at[s3, :, self.relc(d)])
                self.give(0, (1, -1))
            elif st == 4:
                total(self.sub(0), fb.at[s3, :, self.relc(0)], rb.at[s3, 0], rb.at[s3, 1], rb.at[s3, 2])
                self.give(1, PEERS)
            elif st == 5:
                even = self.sub(0)[...].astype(F32) + rc[s6, 1].astype(F32)
                odd = rc[s6, 0].astype(F32) + rc[s6, 2].astype(F32)
                self.sub(0)[...] = (even + odd).astype(BF16)
                self.take(1, 3)
            elif st == 6:
                self.take(0, 2)
            if st <= 7:
                self.send(st)
            else:
                pl.semaphore_wait(free.at[2, 0, s6], 1)
                self.send_mine().start()

    def slot(t, t6, half):
        for st in range(8, 1, -1):
            off = OFF[st]
            if half == 1 and off % 2 == 0:
                back = off // 2
            elif half == 0 and off % 2 == 1:
                back = (1 + off) // 2
            else:
                continue
            u, u6 = t - back, t6 - back % 6

            @pl.when(jnp.logical_and(u >= 0, u < CH))
            def _():
                Chunk(u, jnp.where(u6 < 0, u6 + 6, u6)).stage(st)

    def body(t, t6):
        c = Chunk(t, t6)

        @pl.when(t < CH)
        def _():
            @pl.when(t + 1 < CH)
            def _():
                gcopy(t + 1).start()
            gcopy(t).wait()

            @pl.when(c.col == 0)
            def _():
                acopy(c.n, theirs).wait()

            out[c.n, pl.ds(theirs, H), pl.ds(c.col, NB)] = dot(c.n, t, theirs).astype(BF16)
            c.send_theirs().start()

        slot(t, t6, 0)

        @pl.when(t < CH)
        def _():
            @pl.when(c.col == 0)
            def _():
                acopy(c.n, mine).wait()

            @pl.when(t == 1)
            def _():
                acopy(1, theirs).start()
                acopy(1, mine).start()

            fs[c.s3] = dot(c.n, t, mine)
            w = c.send_theirs()
            w.wait_send()
            pl.semaphore_signal(free.at[2, 0, c.s6], inc=1, device_id={"dp": partner},
                                device_id_type=pl.DeviceIdType.MESH)
            w.wait_recv()
            total(c.block(2), *c.chip(2))
            c.send(1)

        slot(t, t6, 1)
        return jnp.where(t6 == 5, 0, t6 + 1)

    lax.fori_loop(0, LAST, body, 0)

    def drain(t, _):
        c = Chunk(t, 0).send_mine()
        c.wait_send()
        c.wait_recv()
        return 0

    lax.fori_loop(0, CH, drain, 0)


def local(a, g):
    dma = pltpu.SemaphoreType.DMA
    return pl.pallas_call(
        kernel,
        out_shape=pltpu.VMEM((N, D, F), BF16),
        in_specs=[pl.BlockSpec(memory_space=pl.ANY)] * 2,
        out_specs=pl.BlockSpec(memory_space=pltpu.VMEM),
        scratch_shapes=[
            pltpu.VMEM((N, K, D), BF16),
            pltpu.VMEM((2, K, NB), BF16),
            pltpu.VMEM((3, H, NB), F32),
            pltpu.VMEM((3, RB, NB), F32),
            pltpu.VMEM((6, H, NB), BF16),
            pltpu.VMEM((3, RB, NB), BF16),
            pltpu.VMEM((3, 2, RB, NB), BF16),
            pltpu.VMEM((3, 3, RB, CB), BF16),
            pltpu.VMEM((6, 3, RB, CB), BF16),
            dma((2, 2)), dma((2,)), dma((6,)), dma((6,)), dma((CH,)), dma((CH,)),
            dma((7, 3, 6)), dma((7, 3, 6)), pltpu.SemaphoreType.REGULAR((3, 3, 6)),
        ],
        compiler_params=pltpu.CompilerParams(
            collective_id=0, has_side_effects=True, vmem_limit_bytes=46 * 2**20),
        name="wgrad_sum",
    )(a, g)


def solution(mesh):
    spec = P(("rep", "dp"))
    return jax.shard_map(local, mesh=mesh, in_specs=(spec, spec), out_specs=P("rep"), check_vma=False)
```
